32 devices in a mesh: dp: 4 (over x, y), tp: 8 (over z, core).
Axes of the slice: x: 2, y: 2, z: 4, core: 2. Of those that a mesh axis runs over, the one named last changes fastest.
Arguments:
- x: bfloat16 [512, 8192], P('dp'), parts along dimension 0
- w_gate: bfloat16 [8192, 32768], P(None, 'tp')
- w_up: bfloat16 [8192, 32768], P(None, 'tp')
- w_down: bfloat16 [32768, 8192], P('tp')
Outputs:
- output: bfloat16 [512, 8192], P('dp'), parts along dimension 0
There are 4 independent parts. The reference program is written for one: setup_inputs(seed, part) draws one part's arguments, and reference() takes and returns one part's arrays. A program takes and returns all parts, laid end to end along the dimension named above; an argument that names none is the same for every part.
All inputs are finite; a program needn't handle non-finite values.
Results may differ from the reference program's by a relative error of at most 0.016.
Values are sent between devices in bfloat16 or wider.
A program may use at most 2 GiB of HBM per device.

```python
import jax
import jax.numpy as jnp

ROWS = 128
D = 8192
FF = 32768


def setup_inputs(seed: int = 0, part: int = 0) -> dict:
    kx, kg, ku, kd = jax.random.split(jax.random.key(seed), 4)
    drawn = {
        "x": jax.random.normal(jax.random.fold_in(kx, part), (ROWS, D), jnp.float32),
        "w_gate": jax.random.normal(kg, (D, FF), jnp.float32) * D**-0.5,
        "w_up": jax.random.normal(ku, (D, FF), jnp.float32) * D**-0.5,
        "w_down": jax.random.normal(kd, (FF, D), jnp.float32) * FF**-0.5,
    }
    return {k: v.astype(jnp.bfloat16) for k, v in drawn.items()}


def reference(x, w_gate, w_up, w_down):
    gate = jnp.dot(x, w_gate, preferred_element_type=jnp.float32)
    up = jnp.dot(x, w_up, preferred_element_type=jnp.float32)
    hidden = (jax.nn.silu(gate) * up).astype(jnp.bfloat16)
    return jnp.dot(hidden, w_down, preferred_element_type=jnp.float32).astype(jnp.bfloat16)
```

```python
import functools

import jax
import jax.numpy as jnp
from jax import lax
from jax.experimental import pallas as pl
from jax.experimental.pallas import tpu as pltpu
from jax.sharding import PartitionSpec as P

MESH = pl.DeviceIdType.MESH
BF16 = jnp.bfloat16
F32 = jnp.float32

KC = 512
NB = 5
NC = 512
ND = 6
PB = 4

PAIR, OUTER, INNER, MID, BACK, LAST = 2, 7, 11, 15, 19, 21


def kernel(
    x, wg, wu, wd, out,
    xb, gbuf, ubuf, dbuf, accg, accu, hid, pbuf, qbuf,
    send_p, recv_p, send_q, recv_q, send_z, recv_o, recv_m, fin, finp,
    sem_x, sem_g, sem_u, sem_d, sem_out, sem_outp,
    ss_x, rs_x, ss_y, rs_y, ss_f, rs_f,
    ss_p, rs_p, ss_qx, rs_qx, ss_qy, rs_qy,
    ss_z, rs_o, rs_m, ss_b, ss_fp, rs_fp,
):
    rows, d = x.shape
    half = rows // 2
    ff = wg.shape[1] // 2
    nk, nn = d // KC, d // NC
    hk, hn = KC // 2, NC // 2

    dp, tp = lax.axis_index("dp"), lax.axis_index("tp")
    z, core = tp // 2, tp % 2
    xn, yn = (dp + 2) % 4, dp + 1 - 2 * (dp % 2)
    mine = ((dp // 2 + dp) % 2) * ff
    pair = z * 2 + 1 - core
    near = (z + 1 - 2 * (z % 2)) * 2 + core
    across = (3 - z) * 2 + core
    inner = jnp.logical_or(z == 1, z == 2)
    outer = jnp.logical_not(inner)

    def gate_copy(k):
        slot = k % NB
        at = (pl.ds(pl.multiple_of(k * KC, KC), KC), pl.ds(pl.multiple_of(mine, ff), ff))
        return (
            pltpu.make_async_copy(wg.at[at], gbuf.at[slot], sem_g.at[slot]),
            pltpu.make_async_copy(wu.at[at], ubuf.at[slot], sem_u.at[slot]),
        )

    def down_copy(n):
        slot = n % ND
        at = (pl.ds(pl.multiple_of(mine, ff), ff), pl.ds(pl.multiple_of(n * NC, NC), NC))
        return pltpu.make_async_copy(wd.at[at], dbuf.at[slot], sem_d.at[slot])

    def remote(src, dst, ss, rs, **device):
        return pltpu.make_async_remote_copy(
            src_ref=src, dst_ref=dst, send_sem=ss, recv_sem=rs, device_id=device, device_id_type=MESH
        )

    def cols(k, c, width):
        return pl.ds(pl.multiple_of(k * 2 * width + c * width, width), width)

    def token_copies(k):
        at = cols(k, core, hk)
        return (
            remote(xb.at[pl.ds(0, half), at], xb.at[pl.ds(rows, half), at], ss_x.at[k], rs_x.at[k], dp=xn),
            remote(xb.at[pl.ds(half, half), at], xb.at[pl.ds(rows + half, half), at], ss_y.at[k], rs_y.at[k], dp=yn),
        )

    def pass_on(k):
        at = (pl.ds(rows, rows), cols(k, core, hk))
        return remote(xb.at[at], xb.at[at], ss_f.at[k], rs_f.at[k], tp=pair)

    def pair_copy(i):
        return remote(send_p.at[i], recv_p.at[i], ss_p.at[i], rs_p.at[i], tp=pair)

    def home_copies(i):
        return (
            remote(send_q.at[i, pl.ds(0, half)], recv_q.at[i, pl.ds(0, half)], ss_qx.at[i], rs_qx.at[i], dp=xn),
            remote(send_q.at[i, pl.ds(half, half)], recv_q.at[i, pl.ds(half, half)], ss_qy.at[i], rs_qy.at[i], dp=yn),
        )

    def in_copy(i):
        return remote(send_z.at[i], recv_o.at[i], ss_z.at[i], rs_o.at[i], tp=near)

    def mid_copy(i):
        return remote(send_z.at[i], recv_m.at[i], ss_z.at[i], rs_m.at[i], tp=across)

    def back_copy(i):
        return remote(fin.at[i], fin.at[i], ss_b.at[i], rs_o.at[i], tp=near)

    def share_copy(i):
        return remote(fin.at[i], finp.at[i], ss_fp.at[i], rs_fp.at[i], tp=pair)

    def out_copy(i):
        return pltpu.make_async_copy(fin.at[i], out.at[:, cols(i, core, hn)], sem_out.at[i])

    def outp_copy(i):
        return pltpu.make_async_copy(finp.at[i], out.at[:, cols(i, 1 - core, hn)], sem_outp.at[i])

    def loop(n, body):
        lax.fori_loop(0, n, lambda i, c: (body(i), c)[1], 0)

    own = pltpu.make_async_copy(x, xb.at[pl.ds(0, rows)], sem_x)
    own.start()
    for k in range(NB):
        for copy in gate_copy(k):
            copy.start()

    barrier = pltpu.get_barrier_semaphore()
    for device in ({"dp": xn}, {"dp": yn}, {"tp": pair}, {"tp": near}):
        pl.semaphore_signal(barrier, inc=1, device_id=device, device_id_type=MESH)

    @pl.when(inner)
    def _():
        pl.semaphore_signal(barrier, inc=1, device_id={"tp": across}, device_id_type=MESH)

    own.wait()

    @pl.when(outer)
    def _():
        pl.semaphore_wait(barrier, 4)

    @pl.when(inner)
    def _():
        pl.semaphore_wait(barrier, 5)

    @functools.partial(loop, nk)
    def _(k):
        for copy in token_copies(k):
            copy.start()

    accg[...] = jnp.zeros_like(accg)
    accu[...] = jnp.zeros_like(accu)

    def arrive(k):
        for copy in token_copies(k):
            copy.wait_recv()
        pass_on(k).start()

    arrive(0)

    def tokens(k):
        return xb[:, pl.ds(pl.multiple_of(k * KC, KC), KC)]

    @functools.partial(loop, nk - 1)
    def _(k):
        arrive(k + 1)
        pass_on(k).wait_recv()
        for copy in gate_copy(k):
            copy.wait()
        slot = k % NB
        accg[...] += jnp.dot(tokens(k), gbuf[slot], preferred_element_type=F32)
        accu[...] += jnp.dot(tokens(k), ubuf[slot], preferred_element_type=F32)

        @pl.when(k + NB < nk)
        def _():
            for copy in gate_copy(k + NB):
                copy.start()

        for j in range(2):
            n = (k - (nk - NB)) * 2 + j

            @pl.when(jnp.logical_and(n >= 0, n < ND))
            def _():
                down_copy(n).start()

    pass_on(nk - 1).wait_recv()
    for copy in gate_copy(nk - 1):
        copy.wait()
    slot = (nk - 1) % NB
    for j in range(ff // 512):
        at = pl.ds(j * 512, 512)
        gate = accg[:, at] + jnp.dot(tokens(nk - 1), gbuf[slot, :, at], preferred_element_type=F32)
        up = accu[:, at] + jnp.dot(tokens(nk - 1), ubuf[slot, :, at], preferred_element_type=F32)
        hid[:, at] = (jax.nn.silu(gate) * up).astype(BF16)

    def stage(j, lag, body, when=None):
        i = j - lag
        ok = jnp.logical_and(i >= 0, i < nn)
        pl.when(ok if when is None else jnp.logical_and(ok, when))(lambda: body(i))

    def down(i):
        down_copy(i).wait()
        p = jnp.dot(hid[...], dbuf[i % ND], preferred_element_type=F32)
        slot = i % PB
        pbuf[slot, 0] = p[:, :hn]
        pbuf[slot, 1] = p[:, hn:]
        send_p[i] = pbuf[slot, 1 - core].astype(BF16)
        pair_copy(i).start()

        @pl.when(i + ND < nn)
        def _():
            down_copy(i + ND).start()

    def pair_sum(i):
        pair_copy(i).wait_recv()
        slot = i % PB
        send_q[i] = (pbuf[slot, core, rows:, :] + recv_p[i, rows:, :].astype(F32)).astype(BF16)
        for copy in home_copies(i):
            copy.start()
        qbuf[i] = pbuf[slot, core, :rows, :] + recv_p[i, :rows, :].astype(F32)

    def home_sum(i):
        for copy in home_copies(i):
            copy.wait_recv()
        return qbuf[i] + recv_q[i].astype(F32)

    def outer_send(i):
        send_z[i] = home_sum(i).astype(BF16)
        in_copy(i).start()

    def inner_send(i):
        total = home_sum(i)
        in_copy(i).wait_recv()
        send_z[i] = (total + recv_o[i].astype(F32)).astype(BF16)
        mid_copy(i).start()

    def finish(i):
        share_copy(i).start()
        out_copy(i).start()

    def inner_finish(i):
        mid_copy(i).wait_recv()
        fin[i] = (send_z[i].astype(F32) + recv_m[i].astype(F32)).astype(BF16)
        back_copy(i).start()
        finish(i)

    def outer_finish(i):
        back_copy(i).wait_recv()
        finish(i)

    def last(i):
        share_copy(i).wait_recv()
        outp_copy(i).start()

    @functools.partial(loop, nn + LAST)
    def _(j):
        stage(j, 0, down)
        stage(j, PAIR, pair_sum)
        stage(j, OUTER, outer_send, outer)
        stage(j, INNER, inner_send, inner)
        stage(j, MID, inner_finish, inner)
        stage(j, BACK, outer_finish, outer)
        stage(j, LAST, last)

    @functools.partial(loop, nk)
    def _(k):
        for copy in token_copies(k):
            copy.wait_send()
        pass_on(k).wait_send()

    @functools.partial(loop, nn)
    def _(i):
        pair_copy(i).wait_send()
        for copy in home_copies(i):
            copy.wait_send()
        share_copy(i).wait_send()
        out_copy(i).wait()
        outp_copy(i).wait()

        @pl.when(inner)
        def _():
            mid_copy(i).wait_send()
            back_copy(i).wait_send()

        @pl.when(outer)
        def _():
            in_copy(i).wait_send()


def solution(mesh):
    def step(x, w_gate, w_up, w_down):
        rows, d = x.shape
        ff = w_gate.shape[1] // 2
        nk, nn, hn = d // KC, d // NC, NC // 2
        dma = pltpu.SemaphoreType.DMA
        any_space = pl.BlockSpec(memory_space=pl.ANY)
        flops = 2 * 3 * 2 * rows * d * ff
        return pl.pallas_call(
            kernel,
            name="mlp_sum",
            out_shape=jax.ShapeDtypeStruct((rows, d), BF16),
            in_specs=[any_space] * 4,
            out_specs=any_space,
            scratch_shapes=[
                pltpu.VMEM((2 * rows, d), BF16),
                pltpu.VMEM((NB, KC, ff), BF16),
                pltpu.VMEM((NB, KC, ff), BF16),
                pltpu.VMEM((ND, ff, NC), BF16),
                pltpu.VMEM((2 * rows, ff), F32),
                pltpu.VMEM((2 * rows, ff), F32),
                pltpu.VMEM((2 * rows, ff), BF16),
                pltpu.VMEM((PB, 2, 2 * rows, hn), F32),
                pltpu.VMEM((nn, rows, hn), F32),
                pltpu.VMEM((nn, 2 * rows, hn), BF16),
                pltpu.VMEM((nn, 2 * rows, hn), BF16),
                pltpu.VMEM((nn, rows, hn), BF16),
                pltpu.VMEM((nn, rows, hn), BF16),
                pltpu.VMEM((nn, rows, hn), BF16),
                pltpu.VMEM((nn, rows, hn), BF16),
                pltpu.VMEM((nn, rows, hn), BF16),
                pltpu.VMEM((nn, rows, hn), BF16),
                pltpu.VMEM((nn, rows, hn), BF16),
                dma, dma((NB,)), dma((NB,)), dma((ND,)), dma((nn,)), dma((nn,)),
                *[dma((nk,))] * 6,
                *[dma((nn,))] * 12,
            ],
            compiler_params=pltpu.CompilerParams(
                collective_id=0, has_side_effects=True, vmem_limit_bytes=64 * 1024 * 1024 - 65536
            ),
            cost_estimate=pl.CostEstimate(flops=flops, bytes_accessed=3 * d * ff * 2, transcendentals=0),
        )(x, w_gate, w_up, w_down)

    return jax.shard_map(
        step,
        mesh=mesh,
        in_specs=(P("dp", None), P(None, "tp"), P(None, "tp"), P("tp", None)),
        out_specs=P("dp", None),
        check_vma=False,
    )
```

```python
import functools

import jax
import jax.numpy as jnp
from jax import lax
from jax.experimental import pallas as pl
from jax.experimental.pallas import tpu as pltpu
from jax.sharding import PartitionSpec as P

MESH = pl.DeviceIdType.MESH
BF16 = jnp.bfloat16
F32 = jnp.float32

KC = 512
NB = 5
EARLY = 3
NC = 512
ND = 6
PB = 2

SUB = 2
PAIR, OUTER, INNER, MID, BACK, LAST = 2, 8, 14, 19, 26, 28


def kernel(
    x, wg, wu, wd, out,
    xb, gbuf, ubuf, dbuf, accg, accu, hid, pbuf, qbuf,
    send_p, recv_p, send_q, recv_q, send_z, recv_o, recv_m,
    sem_x, sem_g, sem_u, sem_d,
    ss_t, rs_t, ss_f, rs_f,
    ss_p, rs_p, ss_q, rs_q, ss_z, rs_o, rs_m, ss_b, ss_s, rs_s,
):
    rows, d = x.shape
    half = rows // 2
    ff = wg.shape[1] // 2
    nk, nn = d // KC, d // NC
    hk, hn = KC // 2, NC // (2 * SUB)
    ns = nn * SUB

    dp, tp = lax.axis_index("dp"), lax.axis_index("tp")
    z, core = tp // 2, tp % 2
    xn, yn = (dp + 2) % 4, dp + 1 - 2 * (dp % 2)
    mine = ((dp // 2 + dp) % 2) * ff
    pair = z * 2 + 1 - core
    near = (z + 1 - 2 * (z % 2)) * 2 + core
    across = (3 - z) * 2 + core
    inner = jnp.logical_or(z == 1, z == 2)
    outer = jnp.logical_not(inner)

    def gate_copy(k):
        slot = k % NB
        at = (pl.ds(pl.multiple_of(k * KC, KC), KC), pl.ds(pl.multiple_of(mine, ff), ff))
        return (
            pltpu.make_async_copy(wg.at[at], gbuf.at[slot], sem_g.at[slot]),
            pltpu.make_async_copy(wu.at[at], ubuf.at[slot], sem_u.at[slot]),
        )

    def down_copy(n):
        slot = n % ND
        at = (pl.ds(pl.multiple_of(mine, ff), ff), pl.ds(pl.multiple_of(n * NC, NC), NC))
        return pltpu.make_async_copy(wd.at[at], dbuf.at[slot], sem_d.at[slot])

    def remote(src, dst, ss, rs, **device):
        return pltpu.make_async_remote_copy(
            src_ref=src, dst_ref=dst, send_sem=ss, recv_sem=rs, device_id=device, device_id_type=MESH
        )

    def cols(k, c, width):
        return pl.ds(pl.multiple_of(k * 2 * width + c * width, width), width)

    part = pl.ds(pl.multiple_of(core * hk, hk), hk)

    def token_copies(k):
        return (
            remote(xb.at[k, pl.ds(0, half), part], xb.at[k, pl.ds(rows, half), part], ss_t, rs_t.at[k], dp=xn),
            remote(xb.at[k, pl.ds(half, half), part], xb.at[k, pl.ds(rows + half, half), part], ss_t, rs_t.at[k], dp=yn),
        )

    def pass_on(k):
        at = (k, pl.ds(rows, rows), part)
        return remote(xb.at[at], xb.at[at], ss_f, rs_f.at[k], tp=pair)

    def both(k):
        at = (k, pl.ds(rows, rows), part)
        return remote(xb.at[at], xb.at[at], ss_t, rs_t.at[k], dp=xn)

    def pair_copy(i):
        return remote(send_p.at[i], recv_p.at[i], ss_p, rs_p.at[i], tp=pair)

    def home_copies(i):
        x_half, y_half = (i, pl.ds(0, half)), (i, pl.ds(half, half))
        return (
            remote(send_q.at[x_half], recv_q.at[x_half], ss_q, rs_q.at[i], dp=xn),
            remote(send_q.at[y_half], recv_q.at[y_half], ss_q, rs_q.at[i], dp=yn),
        )

    def in_copy(i):
        return remote(send_z.at[i], recv_o.at[i], ss_z, rs_o.at[i], tp=near)

    def mid_copy(i):
        return remote(send_z.at[i], recv_m.at[i], ss_z, rs_m.at[i], tp=across)

    def back_copy(i):
        at = (slice(None), cols(i, core, hn))
        return remote(out.at[at], out.at[at], ss_b, rs_o.at[i], tp=near)

    def share_copy(i):
        at = (slice(None), cols(i, core, hn))
        return remote(out.at[at], out.at[at], ss_s, rs_s.at[i], tp=pair)

    def loop(n, body):
        lax.fori_loop(0, n, lambda i, c: (body(i), c)[1], 0)

    barrier = pltpu.get_barrier_semaphore()
    for device in ({"dp": xn}, {"dp": yn}, {"tp": pair}, {"tp": near}):
        pl.semaphore_signal(barrier, inc=1, device_id=device, device_id_type=MESH)

    @pl.when(inner)
    def _():
        pl.semaphore_signal(barrier, inc=1, device_id={"tp": across}, device_id_type=MESH)

    @functools.partial(loop, nk)
    def _(k):
        at = pl.ds(pl.multiple_of(k * KC, KC), KC)
        pltpu.make_async_copy(x.at[:, at], xb.at[k, pl.ds(0, rows)], sem_x).start()

    for k in range(NB):
        for copy in gate_copy(k):
            copy.start()

    accg[...] = jnp.zeros_like(accg)
    accu[...] = jnp.zeros_like(accu)

    own = xb.at[:, pl.ds(0, rows)]
    pltpu.make_async_copy(own, own, sem_x).wait()

    @pl.when(outer)
    def _():
        pl.semaphore_wait(barrier, 4)

    @pl.when(inner)
    def _():
        pl.semaphore_wait(barrier, 5)

    @functools.partial(loop, nk)
    def _(k):
        for copy in token_copies(k):
            copy.start()

    def arrive(k):
        both(k).wait_recv()
        pass_on(k).start()

    def weights(k):
        for copy in gate_copy(k):
            copy.wait()

    def gate_up(k, at):
        slot = k % NB
        accg[at] += jnp.dot(xb[k, at], gbuf[slot], preferred_element_type=F32)
        accu[at] += jnp.dot(xb[k, at], ubuf[slot], preferred_element_type=F32)

    def refill(k):
        @pl.when(k + NB < nk)
        def _():
            for copy in gate_copy(k + NB):
                copy.start()

        for j in range(2):
            n = (k - (nk - NB)) * 2 + j

            @pl.when(jnp.logical_and(n >= 0, n < ND))
            def _():
                down_copy(n).start()

    @functools.partial(loop, EARLY)
    def _(k):
        weights(k)
        gate_up(k, pl.ds(0, rows))
        pl.when(k >= 1)(lambda: arrive(k - 1))

    arrive(EARLY - 1)

    @functools.partial(loop, EARLY)
    def _(k):
        arrive(k + EARLY)
        pass_on(k).wait_recv()
        gate_up(k, pl.ds(rows, rows))
        refill(k)

    @functools.partial(loop, nk - 1 - EARLY)
    def _(j):
        k = j + EARLY
        pl.when(k + EARLY < nk)(lambda: arrive(k + EARLY))
        pass_on(k).wait_recv()
        weights(k)
        gate_up(k, pl.ds(0, 2 * rows))
        refill(k)

    pass_on(nk - 1).wait_recv()
    weights(nk - 1)
    slot = (nk - 1) % NB
    for j in range(ff // 512):
        at = pl.ds(j * 512, 512)
        gate = accg[:, at] + jnp.dot(xb[nk - 1], gbuf[slot, :, at], preferred_element_type=F32)
        up = accu[:, at] + jnp.dot(xb[nk - 1], ubuf[slot, :, at], preferred_element_type=F32)
        hid[:, at] = (jax.nn.silu(gate) * up).astype(BF16)

    def stage(j, lag, body, when=None, n=ns):
        i = j - lag
        ok = jnp.logical_and(i >= 0, i < n)
        pl.when(ok if when is None else jnp.logical_and(ok, when))(lambda: body(i))

    def down(i):
        down_copy(i).wait()
        p = jnp.dot(hid[...], dbuf[i % ND], preferred_element_type=F32)
        for u in range(SUB):
            for c in range(2):
                pbuf[i % PB, u, c] = p[:, (2 * u + c) * hn : (2 * u + c + 1) * hn]
            send_p[SUB * i + u] = pbuf[i % PB, u, 1 - core].astype(BF16)
            pair_copy(SUB * i + u).start()

        @pl.when(i + ND < nn)
        def _():
            down_copy(i + ND).start()

    def pair_sum(i):
        pair_copy(i).wait_recv()
        mine_p = pbuf.at[(i // SUB) % PB, i % SUB, core]
        send_q[i] = (mine_p[rows:, :] + recv_p[i, rows:, :].astype(F32)).astype(BF16)
        for copy in home_copies(i):
            copy.start()
        qbuf[i] = mine_p[:rows, :] + recv_p[i, :rows, :].astype(F32)

    def home_sum(i):
        remote(send_q.at[i], recv_q.at[i], ss_q, rs_q.at[i], dp=xn).wait_recv()
        return qbuf[i] + recv_q[i].astype(F32)

    def outer_send(i):
        send_z[i] = home_sum(i).astype(BF16)
        in_copy(i).start()

    def inner_send(i):
        total = home_sum(i)
        in_copy(i).wait_recv()
        send_z[i] = (total + recv_o[i].astype(F32)).astype(BF16)
        mid_copy(i).start()

    def inner_finish(i):
        mid_copy(i).wait_recv()
        out[:, cols(i, core, hn)] = (send_z[i].astype(F32) + recv_m[i].astype(F32)).astype(BF16)
        back_copy(i).start()
        share_copy(i).start()

    def outer_finish(i):
        back_copy(i).wait_recv()
        share_copy(i).start()

    def last(i):
        share_copy(i).wait_recv()

    @functools.partial(loop, nn + (LAST + SUB - 1) // SUB)
    def _(j):
        stage(j, 0, down, n=nn)
        for u in range(SUB):
            i = SUB * j + u
            stage(i, PAIR, pair_sum)
            stage(i, OUTER, outer_send, outer)
            stage(i, INNER, inner_send, inner)
            stage(i, MID, inner_finish, inner)
            stage(i, BACK, outer_finish, outer)
            stage(i, LAST, last)

    tokens = xb.at[:, pl.ds(rows, rows), pl.ds(0, hk)]

    def sent(ref, ss):
        remote(ref, ref, ss, rs_p.at[0], tp=pair).wait_send()

    sent(tokens, ss_t)
    sent(tokens, ss_f)
    sent(send_p, ss_p)
    sent(send_q, ss_q)
    sent(send_z, ss_z)
    sent(send_z, ss_s)

    @pl.when(inner)
    def _():
        sent(send_z, ss_b)


def solution(mesh):
    def step(x, w_gate, w_up, w_down):
        rows, d = x.shape
        ff = w_gate.shape[1] // 2
        nk, ns, hn = d // KC, d // NC * SUB, NC // (2 * SUB)
        dma = pltpu.SemaphoreType.DMA
        any_space = pl.BlockSpec(memory_space=pl.ANY)
        flops = 2 * 3 * 2 * rows * d * ff
        return pl.pallas_call(
            kernel,
            name="mlp_sum",
            out_shape=pltpu.VMEM((rows, d), BF16),
            in_specs=[any_space] * 4,
            out_specs=pl.BlockSpec(memory_space=pltpu.VMEM),
            scratch_shapes=[
                pltpu.VMEM((nk, 2 * rows, KC), BF16),
                pltpu.VMEM((NB, KC, ff), BF16),
                pltpu.VMEM((NB, KC, ff), BF16),
                pltpu.VMEM((ND, ff, NC), BF16),
                pltpu.VMEM((2 * rows, ff), F32),
                pltpu.VMEM((2 * rows, ff), F32),
                pltpu.VMEM((2 * rows, ff), BF16),
                pltpu.VMEM((PB, SUB, 2, 2 * rows, hn), F32),
                pltpu.VMEM((ns, rows, hn), F32),
                pltpu.VMEM((ns, 2 * rows, hn), BF16),
                pltpu.VMEM((ns, 2 * rows, hn), BF16),
                pltpu.VMEM((ns, rows, hn), BF16),
                pltpu.VMEM((ns, rows, hn), BF16),
                pltpu.VMEM((ns, rows, hn), BF16),
                pltpu.VMEM((ns, rows, hn), BF16),
                pltpu.VMEM((ns, rows, hn), BF16),
                dma, dma((NB,)), dma((NB,)), dma((ND,)),
                dma, dma((nk,)), dma, dma((nk,)),
                dma, dma((ns,)), dma, dma((ns,)), dma, dma((ns,)), dma((ns,)), dma, dma, dma((ns,)),
            ],
            compiler_params=pltpu.CompilerParams(
                collective_id=0, has_side_effects=True, vmem_limit_bytes=60 * 1024 * 1024
            ),
            cost_estimate=pl.CostEstimate(flops=flops, bytes_accessed=3 * d * ff * 2, transcendentals=0),
        )(x, w_gate, w_up, w_down)

    return jax.shard_map(
        step,
        mesh=mesh,
        in_specs=(P("dp", None), P(None, "tp"), P(None, "tp"), P("tp", None)),
        out_specs=P("dp", None),
        check_vma=False,
    )
```
